256 devices in a mesh: expert: 128 (over y_lo, z, x, core), dp: 2 (over y_hi).
Axes of the slice: x: 4, y: 4 (y_hi: 2, y_lo: 2; y = y_hi * 2 + y_lo), z: 8, core: 2. Of those that a mesh axis runs over, the one named last changes fastest.
Arguments:
- tokens: bfloat16 [32768, 2560], P(('expert', 'dp')), may hold values from -6 to 6
- routes: int32 [32768, 6], P(('expert', 'dp')), may hold values from 0 to 31, all different within a row; in each aligned block of 128 rows (0 to 127, 128 to 255, ...) at most 32 rows name the same one
- combine_weight: float32 [32768, 6], P(('expert', 'dp')), may hold values from 0.05 to 1
- owner_plan: int32 [32], replicated, may hold values from 0 to 31, as said below
- w_in: bfloat16 [2, 24576, 2560], P(None, 'expert', 'dp'), may hold values from -0.125 to 0.125
- w_out: bfloat16 [24576, 2560], P('expert', 'dp'), may hold values from -0.21875 to 0.21875
- grad_in: bfloat16 [2, 2, 24576, 2560], P('dp', None, 'expert'), may hold values from -6 to 6
- grad_out: bfloat16 [2, 24576, 2560], P('dp', 'expert'), may hold values from -6 to 6
- first_in: bfloat16 [2, 24576, 2560], P(None, 'expert', 'dp'), may hold values from -3 to 3
- second_in: bfloat16 [2, 24576, 2560], P(None, 'expert', 'dp'), may hold values from 0.25 to 4
- first_out: bfloat16 [24576, 2560], P('expert', 'dp'), may hold values from -3 to 3
- second_out: bfloat16 [24576, 2560], P('expert', 'dp'), may hold values from 0.25 to 4
Outputs:
- combined: bfloat16 [32768, 2560], P(('expert', 'dp'))
- first_in_next: bfloat16 [2, 24576, 2560], P(None, 'expert', 'dp')
- second_in_next: bfloat16 [2, 24576, 2560], P(None, 'expert', 'dp')
- first_out_next: bfloat16 [24576, 2560], P('expert', 'dp')
- second_out_next: bfloat16 [24576, 2560], P('expert', 'dp')
The draws below stay inside these ranges and needn't reach their ends.
Inputs may be any that keep to these rules, and one draw needn't show every extreme that they name: owner_plan is an involution: exactly 4 pairs of experts trade owners, every other expert maps to itself. `routes`: in the rows of one device (128 rows) no expert is named by more than 32 rows, a bound that some expert reaches in some device.
All inputs are finite; a program needn't handle non-finite values.
Results may differ from the reference program's by a relative error of at most 0.014.
Values may be sent and summed in bfloat16 or wider, within the bound.
No kernel may reach another device: no remote copies, remote signals or barrier semaphores. Data moves between devices by JAX's collectives and lax.ppermute only.
A program may use at most 192 MiB of HBM per device.

```python
import math
import jax
import jax.numpy as jnp
import numpy as np
from jax import lax

D = 2560
HID = 768
GROUP = 4
TOK_DEV = 128
HDEV = 192
EXPERTS = 32
TOP = 6
MOVED = 4
CAP = 32
TOKENS = 32768
N_DP = 2
DEVICES = 256


def draw_owner_plan(key, part):
    shuffled = jax.random.permutation(jax.random.fold_in(key, 7), EXPERTS).astype(jnp.int32)
    expert_ids = jnp.arange(EXPERTS, dtype=jnp.int32)
    leaving = shuffled[:MOVED]
    arriving = shuffled[MOVED:2 * MOVED]
    owner_plan = expert_ids.at[leaving].set(arriving).at[arriving].set(leaving)
    return owner_plan.astype(jnp.int32)


def shard_levels(stream_key, dims, cuts, low, top_value):
    factor_of = 1.0
    for axis_at, parts in cuts:
        heights = jax.random.uniform(jax.random.fold_in(jax.random.fold_in(stream_key, 6), axis_at), (parts,), jnp.float32, low / len(cuts), top_value / len(cuts))
        factor_of = factor_of * jnp.repeat(jnp.exp(heights), dims[axis_at] // parts).reshape((-1,) + (1,) * (len(dims) - 1 - axis_at))
    return factor_of


def deal_out(key, own, number, rows, number_of, top, bound, slope):
    order = jax.random.permutation(key, number_of)
    packed, common = portions_of(number_of, rows * top, bound, slope, True), portions_of(number_of, rows * top, bound, slope, False)
    places = jnp.arange(number_of)

    def named(lengths, offset_by):
        used = int((lengths > 0).sum())
        fixed = max(1, used // 4)
        moved = fixed + (places - fixed + offset_by * (used - fixed)) % max(1, number_of - fixed)
        return jnp.zeros((number_of,), jnp.int32).at[order[jnp.where(places < fixed, places, moved)]].set(jnp.asarray(lengths, jnp.int32))

    lengths = jnp.where(number % 4 == 0, named(packed, number // 4), named(common, number - number // 4 - 1))
    mixed = jax.random.permutation(jax.random.fold_in(own, 3), number_of)
    giver, taker = mixed[0:number_of // 2 * 2:2], mixed[1:number_of // 2 * 2:2]
    slack = jnp.minimum(lengths[giver] - 1, bound - lengths[taker]) // 2
    slack = jnp.where((giver == order[0]) | (taker == order[0]) | (lengths[taker] == 0), 0, jnp.maximum(slack, 0))
    moved = jax.random.randint(jax.random.fold_in(own, 4), (number_of // 2,), 0, 1 << 20) % (slack + 1)
    lengths = lengths.at[giver].add(-moved).at[taker].add(moved)
    members = jnp.searchsorted(jnp.cumsum(lengths), jnp.arange(rows * top), side="right").astype(jnp.int32)
    listing = members.reshape(top, rows).T
    listing = listing[jax.random.permutation(jax.random.fold_in(own, 1), rows)]
    offset_by = jax.random.randint(jax.random.fold_in(own, 2), (rows, 1), 0, top)
    return jnp.take_along_axis(listing, (jnp.arange(top)[None, :] + offset_by) % top, axis=1)


def portions_of(amount, total, bound, slope, full):
    loads = [(1 << 20) // math.isqrt(rank ** slope) + 1 for rank in range(1, amount + 1)]
    largest = bound if full else min(bound, max(-(-total // amount), total * loads[0] // sum(loads)))
    least = 1 if total - largest >= amount - 1 else 0
    counts, rest = [largest] + [least] * (amount - 1), total - largest - least * (amount - 1)
    while rest > 0:
        candidates = [i for i in range(1, amount) if counts[i] < largest] or [i for i in range(1, amount) if counts[i] < bound]
        pool, left = sum([loads[i] for i in candidates]), rest
        for i in candidates:
            extra = min(bound - counts[i], max(1, left * loads[i] // pool), rest)
            counts[i] = counts[i] + extra
            rest = rest - extra
    return np.array(counts)


def noise(rng, extent, scale, limit, shards=(), held_as=jnp.bfloat16):
    array = jax.random.normal(rng, extent, jnp.float32) * scale
    if len(shards) > 0:
        array = shard_levels(rng, extent, shards, -0.22, 0.18) * array
    return jnp.clip(array, min=-limit, max=limit).astype(held_as)


def setup_inputs(seed: int = 0) -> dict:
    keys = jax.random.split(jax.random.key(seed), 13)
    tokens = noise(keys[0], (TOKENS, D), 1.0, 6.0, ((0, 256),))
    routes_keys = jax.random.split(jax.random.fold_in(keys[1], 1), TOKENS // TOK_DEV)
    routes_turns = jax.random.permutation(jax.random.fold_in(keys[1], 3), TOKENS // TOK_DEV)
    routes = jax.vmap(lambda own, number: deal_out(jax.random.fold_in(keys[1], 2), own, number, TOK_DEV, EXPERTS, TOP, CAP, 2))(routes_keys, routes_turns).reshape((TOKENS, TOP))
    combine_weight = jnp.clip(jnp.exp(math.log(1.0) - 2.9957323 * jax.random.uniform(keys[2], (TOKENS, TOP), jnp.float32) ** shard_levels(keys[2], (TOKENS, TOP), ((0, 256),), -0.2, 0.2)), 0.05, 1.0)
    owner_plan = draw_owner_plan(jax.random.fold_in(keys[12], 71), 0)
    w_in = noise(keys[4], (2, EXPERTS * HID, D), D ** -0.5, 0.125, ((1, 128), (2, 2)))
    w_out = noise(keys[5], (EXPERTS * HID, D), HID ** -0.5, 0.21875, ((0, 128), (1, 2)))
    grad_in = noise(keys[6], (N_DP, 2, EXPERTS * HID, D), 1.0, 6.0, ((0, 2), (2, 128)))
    grad_out = noise(keys[7], (N_DP, EXPERTS * HID, D), 1.0, 6.0, ((0, 2), (1, 128)))
    first_in = noise(keys[8], (2, EXPERTS * HID, D), 0.5, 3.0, ((1, 128), (2, 2)))
    second_in = jnp.clip(jnp.exp(math.log(4.0) - 2.7725887 * jax.random.uniform(keys[9], (2, EXPERTS * HID, D), jnp.float32) ** shard_levels(keys[9], (2, EXPERTS * HID, D), ((1, 128), (2, 2)), -0.2, 0.2)), 0.25, 4.0).astype(jnp.bfloat16)
    first_out = noise(keys[10], (EXPERTS * HID, D), 0.5, 3.0, ((0, 128), (1, 2)))
    second_out = jnp.clip(jnp.exp(math.log(4.0) - 2.7725887 * jax.random.uniform(keys[11], (EXPERTS * HID, D), jnp.float32) ** shard_levels(keys[11], (EXPERTS * HID, D), ((0, 128), (1, 2)), -0.2, 0.2)), 0.25, 4.0).astype(jnp.bfloat16)
    return dict(tokens=tokens, routes=routes, combine_weight=combine_weight, owner_plan=owner_plan, w_in=w_in, w_out=w_out, grad_in=grad_in, grad_out=grad_out, first_in=first_in, second_in=second_in, first_out=first_out, second_out=second_out)


BETA_ONE = 0.9
BETA_TWO = 0.95
LEARNING_RATE = 0.005
EPSILON = 1e-08
CORRECT_FIRST = 1.0 / (1.0 - 0.9 ** 10)
CORRECT_SECOND = 1.0 / (1.0 - 0.95 ** 10)

def adam_update(weight, gradient, first_moment, second_moment):
    first_next = BETA_ONE * first_moment.astype(jnp.float32) + (1.0 - BETA_ONE) * gradient
    second_next = BETA_TWO * second_moment.astype(jnp.float32) + (1.0 - BETA_TWO) * gradient * gradient
    stepped = weight.astype(jnp.float32) - LEARNING_RATE * (first_next * CORRECT_FIRST) / (jnp.sqrt(second_next * CORRECT_SECOND) + EPSILON)
    return (stepped.astype(jnp.bfloat16), first_next.astype(jnp.bfloat16), second_next.astype(jnp.bfloat16))

def slot_ranks(flat_routes):
    onehot = (flat_routes[:, None] == jnp.arange(EXPERTS, dtype=jnp.int32)[None, :]).astype(jnp.int32)
    ranks = jnp.cumsum(onehot, axis=0) - 1
    return lax.optimization_barrier(jnp.sum(ranks * onehot, axis=1)).astype(jnp.int32)

def times_rows(row_data, weight_rows):
    return lax.dot_general(row_data, weight_rows, (((1,), (1,)), ((), ())), preferred_element_type=jnp.float32)

def expert_rows(row_data, weight_in, weight_out):
    gate = times_rows(row_data, weight_in[0])
    upward = times_rows(row_data, weight_in[1])
    hidden = (jax.nn.silu(gate) * upward).astype(jnp.bfloat16)
    return jnp.dot(hidden, weight_out, preferred_element_type=jnp.float32).astype(jnp.bfloat16)

def expert_output(row_data, weight_in, weight_out):
    total = jnp.zeros((row_data.shape[0], weight_out.shape[1]), jnp.float32)
    for quarter in range(GROUP):
        begin = quarter * HDEV
        total = total + expert_rows(row_data, weight_in[:, begin:begin + HDEV], weight_out[begin:begin + HDEV]).astype(jnp.float32)
    return total.astype(jnp.bfloat16)

def reference(tokens, routes, combine_weight, owner_plan, w_in, w_out, grad_in, grad_out, first_in, second_in, first_out, second_out):
    width = tokens.shape[1]
    sum_in = lax.optimization_barrier(jnp.sum(grad_in.astype(jnp.float32), axis=0))
    sum_out = lax.optimization_barrier(jnp.sum(grad_out.astype(jnp.float32), axis=0))
    new_in, first_in_next, second_in_next = adam_update(w_in, sum_in, first_in, second_in)
    new_out, first_out_next, second_out_next = adam_update(w_out, sum_out, first_out, second_out)

    def regroup_in(moment):
        return jnp.take(moment.reshape(2, EXPERTS, HID, width), owner_plan, axis=1).reshape(moment.shape)

    def regroup_out(moment):
        return jnp.take(moment.reshape(EXPERTS, HID, width), owner_plan, axis=0).reshape(moment.shape)
    device_routes = routes.reshape(DEVICES, TOK_DEV * TOP)
    ranks = jax.vmap(slot_ranks)(device_routes)
    targets = (device_routes * CAP + ranks).astype(jnp.int32)
    token_ids = jnp.arange(TOKENS, dtype=jnp.int32).reshape(DEVICES, TOK_DEV)
    token_of_route = jnp.repeat(token_ids, TOP, axis=1)
    device_ids = jnp.repeat(jnp.arange(DEVICES, dtype=jnp.int32)[:, None], TOK_DEV * TOP, axis=1)
    table = jnp.zeros((DEVICES, EXPERTS * CAP), jnp.int32).at[device_ids, targets].set(token_of_route)
    weight_table = jnp.zeros((DEVICES, EXPERTS * CAP), jnp.float32).at[device_ids, targets].set(combine_weight.reshape(DEVICES, TOK_DEV * TOP))

    def one_expert(total, expert):
        start = (expert * CAP).astype(jnp.int32)
        row_ids = lax.dynamic_slice_in_dim(table, start, CAP, 1).reshape(-1)
        row_weights = lax.dynamic_slice_in_dim(weight_table, start, CAP, 1).reshape(-1)
        weight_in = lax.dynamic_slice_in_dim(new_in, (expert * HID).astype(jnp.int32), HID, 1)
        weight_out = lax.dynamic_slice_in_dim(new_out, (expert * HID).astype(jnp.int32), HID, 0)
        result = expert_output(tokens[row_ids], weight_in, weight_out)
        return (total.at[row_ids].add(row_weights[:, None] * result.astype(jnp.float32)), None)
    total, ignored = lax.scan(one_expert, jnp.zeros((TOKENS, width), jnp.float32), jnp.arange(EXPERTS, dtype=jnp.int32))
    return (total.astype(jnp.bfloat16), regroup_in(first_in_next), regroup_in(second_in_next), regroup_out(first_out_next), regroup_out(second_out_next))
```

```python
import jax
import jax.numpy as jnp
from jax import lax
from jax.experimental import pallas as pl
from jax.experimental.pallas import tpu as pltpu
from jax.sharding import Mesh
from jax.sharding import PartitionSpec as P


BETA_ONE = 0.9
BETA_TWO = 0.95
LEARNING_RATE = 0.005
EPSILON = 1e-08
CORRECT_FIRST = 1.0 / (1.0 - 0.9**10)
CORRECT_SECOND = 1.0 / (1.0 - 0.95**10)

YL, NZ, XP, XQ, CORES, NDP = 2, 8, 2, 2, 2, 2
AXES = ("yl", "z", "xp", "xq", "c", "dp")
TOK, TOP, D, HALF, HDEV, CAP = 128, 6, 2560, 1280, 192, 32
ROWS = NZ * CAP
HID = 4 * HDEV
SWAP = [(0, 1), (1, 0)]
X_FAR = [(0, 3), (3, 0), (1, 2), (2, 1)]
DIAGONAL = [(yl * 4 + a, (1 - yl) * 4 + b) for yl in range(2) for a, b in X_FAR]

BF16, F32 = jnp.bfloat16, jnp.float32


def to_x(a):
    return lax.ppermute(a, ("xp", "xq"), X_FAR)


def to_y(a):
    return lax.ppermute(a, "yl", SWAP)


def to_diagonal(a):
    return lax.ppermute(a, ("yl", "xp", "xq"), DIAGONAL)


def adam_kernel(d_ref, w_in, w_out, g_in, g_out, got_in, got_out, f_in, s_in, f_out, s_out, new, moments):
    for m in range(3):
        w, ga, gb, f, s = (
            (w_in[m], g_in[0, m], got_in[m], f_in[m], s_in[m])
            if m < 2
            else (w_out[...], g_out[0], got_out[...], f_out[...], s_out[...])
        )
        g = ga.astype(F32) + gb.astype(F32)
        first = BETA_ONE * f.astype(F32) + (1.0 - BETA_ONE) * g
        second = BETA_TWO * s.astype(F32) + (1.0 - BETA_TWO) * g * g
        stepped = w.astype(F32) - LEARNING_RATE * (first * CORRECT_FIRST) / (
            jnp.sqrt(second * CORRECT_SECOND) + EPSILON
        )
        new[m] = stepped.astype(BF16)
        moments[m] = first.astype(BF16)
        moments[3 + m] = second.astype(BF16)


def adam(d, w_in, w_out, g_in, g_out, got_in, got_out, f_in, s_in, f_out, s_out):
    block = 48
    three = pl.BlockSpec((2, block, HALF), lambda i, d: (0, i, 0))
    two = pl.BlockSpec((block, HALF), lambda i, d: (i, 0))
    return pl.pallas_call(
        adam_kernel,
        grid_spec=pltpu.PrefetchScalarGridSpec(
            num_scalar_prefetch=1,
            grid=(HDEV // block,),
            in_specs=[
                three,
                two,
                pl.BlockSpec((1, 2, block, HALF), lambda i, d: (0, 0, i, d[0])),
                pl.BlockSpec((1, block, HALF), lambda i, d: (0, i, d[0])),
                three,
                two,
                three,
                three,
                two,
                two,
            ],
            out_specs=[
                pl.BlockSpec((3, block, HALF), lambda i, d: (0, i, 0)),
                pl.BlockSpec((6, block, HALF), lambda i, d: (0, i, 0)),
            ],
        ),
        out_shape=[
            jax.ShapeDtypeStruct((3, HDEV, HALF), BF16),
            jax.ShapeDtypeStruct((6, HDEV, HALF), BF16),
        ],
        name="adam",
    )(d, w_in, w_out, g_in, g_out, got_in, got_out, f_in, s_in, f_out, s_out)


def select_kernel(sel, tok, *outs):
    rows = jnp.dot(sel[0], tok[0], preferred_element_type=F32).astype(BF16)
    for b, out in enumerate(outs):
        out[0] = rows[b * CAP : (b + 1) * CAP]


def select_rows(sel, tok):
    return pl.pallas_call(
        select_kernel,
        grid=(NZ,),
        in_specs=[
            pl.BlockSpec((1, 4 * CAP, TOK), lambda s: (s, 0, 0)),
            pl.BlockSpec((1, TOK, HALF), lambda s: (s, 0, 0)),
        ],
        out_specs=[pl.BlockSpec((1, CAP, HALF), lambda s: (s, 0, 0))] * 4,
        out_shape=[jax.ShapeDtypeStruct((NZ, CAP, HALF), BF16)] * 4,
        name="select",
    )(sel, tok)


def combine_kernel(high, low, r0, r1, r2, r3, out):
    rows = jnp.concatenate([r0[0], r1[0], r2[0], r3[0]], axis=0)
    dims = (((0,), (0,)), ((), ()))
    total = lax.dot_general(high[0], rows, dims, preferred_element_type=F32)
    total = total + lax.dot_general(low[0], rows, dims, preferred_element_type=F32)
    out[0] = total.astype(BF16)


def combine_rows(high, low, parts):
    return pl.pallas_call(
        combine_kernel,
        grid=(NZ,),
        in_specs=[pl.BlockSpec((1, 4 * CAP, TOK), lambda s: (s, 0, 0))] * 2
        + [pl.BlockSpec((1, CAP, HALF), lambda s: (s, 0, 0))] * 4,
        out_specs=pl.BlockSpec((1, TOK, HALF), lambda s: (s, 0, 0)),
        out_shape=jax.ShapeDtypeStruct((NZ, TOK, HALF), BF16),
        name="combine",
    )(high, low, *parts)


def ffn_kernel(blocks, *refs):
    pieces, rows = refs[:8], refs[8 : 8 + 2 * blocks]
    outs = refs[8 + 2 * blocks : 8 + 4 * blocks]
    weights, held, result, weight_sem, row_sem, out_sem = refs[8 + 4 * blocks :]
    copies = []
    for q in range(4):
        for h in range(2):
            piece = pieces[2 * q + h]
            for m in range(3):
                copies.append(
                    pltpu.make_async_copy(
                        piece.at[m], weights.at[h, m, pl.ds(q * HDEV, HDEV)], weight_sem.at[q, h, m]
                    )
                )
    for i in range(blocks):
        for h in range(2):
            copies.append(
                pltpu.make_async_copy(rows[2 * i + h], held.at[h, pl.ds(i * ROWS, ROWS)], row_sem.at[i, h])
            )
    for copy in copies:
        copy.start()
    for copy in copies:
        copy.wait()
    nt = (((1,), (1,)), ((), ()))

    def one_block(i, carry):
        begin = pl.multiple_of(i * ROWS, ROWS)
        x0, x1 = held[0, pl.ds(begin, ROWS)], held[1, pl.ds(begin, ROWS)]

        def project(m):
            return lax.dot_general(x0, weights[0, m], nt, preferred_element_type=F32) + lax.dot_general(
                x1, weights[1, m], nt, preferred_element_type=F32
            )

        hidden = (jax.nn.silu(project(0)) * project(1)).astype(BF16)
        for h in range(2):
            result[h, pl.ds(begin, ROWS)] = jnp.dot(
                hidden, weights[h, 2], preferred_element_type=F32
            ).astype(BF16)
        return carry

    lax.fori_loop(0, blocks, one_block, 0)
    copies = []
    for i in range(blocks):
        for h in range(2):
            copies.append(
                pltpu.make_async_copy(result.at[h, pl.ds(i * ROWS, ROWS)], outs[2 * i + h], out_sem.at[i, h])
            )
    for copy in copies:
        copy.start()
    for copy in copies:
        copy.wait()


def ffn(pieces, rows):
    blocks = len(rows) // 2
    anywhere = pl.BlockSpec(memory_space=pl.ANY)
    return pl.pallas_call(
        lambda *refs: ffn_kernel(blocks, *refs),
        in_specs=[anywhere] * (8 + 2 * blocks),
        out_specs=[anywhere] * (2 * blocks),
        out_shape=[jax.ShapeDtypeStruct((ROWS, HALF), BF16)] * (2 * blocks),
        scratch_shapes=[
            pltpu.VMEM((2, 3, HID, HALF), BF16),
            pltpu.VMEM((2, blocks * ROWS, HALF), BF16),
            pltpu.VMEM((2, blocks * ROWS, HALF), BF16),
            pltpu.SemaphoreType.DMA((4, 2, 3)),
            pltpu.SemaphoreType.DMA((blocks, 2)),
            pltpu.SemaphoreType.DMA((blocks, 2)),
        ],
        name=f"ffn{blocks}",
    )(*pieces, *rows)


def halves(a, d, axis):
    left, right = jnp.split(a, 2, axis=axis)
    return jnp.where(d == 0, left, right), jnp.where(d == 0, right, left)


def local(tokens, routes, combine_weight, owner_plan, w_in, w_out, grad_in, grad_out, first_in, second_in, first_out, second_out):
    d = lax.axis_index("dp")
    yl, z, xp = lax.axis_index("yl"), lax.axis_index("z"), lax.axis_index("xp")

    tok = [
        lax.all_gather(t, "z", axis=0, tiled=False) for t in halves(tokens, d, 1)
    ]
    listing = jnp.concatenate(
        [
            routes.T.astype(F32),
            jnp.zeros((2, TOK), F32),
            combine_weight.T,
            jnp.zeros((2, TOK), F32),
        ],
        axis=0,
    )
    listings = lax.all_to_all(
        jnp.broadcast_to(listing, (NZ, 16, TOK)), "z", split_axis=0, concat_axis=0, tiled=True
    )

    sent_in = halves(grad_in[0], d, 2)[1]
    sent_out = halves(grad_out[0], d, 1)[1]
    got_in = lax.ppermute(sent_in, "dp", SWAP)
    got_out = lax.ppermute(sent_out, "dp", SWAP)
    new, moments = adam(
        d.reshape(1), w_in, w_out, grad_in, grad_out, got_in, got_out, first_in, second_in, first_out, second_out
    )
    other = lax.ppermute(new, "dp", SWAP)
    near = [new, other]
    far = [lax.ppermute(a, "xq", SWAP) for a in near]
    core_near = [lax.ppermute(a, "c", SWAP) for a in near]
    core_far = [lax.ppermute(a, "c", SWAP) for a in far]
    pieces = near + far + core_near + core_far

    spread = moments.reshape(16, 72, 2, 640).transpose(0, 2, 1, 3).reshape(32, 72, 640)
    spread = lax.all_to_all(spread, ("yl", "z", "xp"), 0, 0, tiled=True)
    picked = jnp.take(spread, owner_plan, axis=0)
    landed = lax.all_to_all(picked, ("yl", "z", "xp"), 0, 0, tiled=True)
    landed = landed.reshape(16, 2, 72, 640).transpose(0, 2, 1, 3).reshape(6, HDEV, HALF)

    experts = jnp.stack(
        [a * 16 + z * 2 + b for a, b in ((yl, xp), (yl, 1 - xp), (1 - yl, xp), (1 - yl, 1 - xp))]
    ).astype(F32)
    named = (listings[:, None, :TOP] == experts[None, :, None, None])
    weight = jnp.sum(jnp.where(named, listings[:, None, 8 : 8 + TOP], 0.0), axis=2)
    named = jnp.any(named, axis=2)
    before = (jnp.arange(TOK)[:, None] < jnp.arange(TOK)[None, :]).astype(BF16)
    rank = jnp.dot(named.astype(BF16).reshape(NZ * 4, TOK), before, preferred_element_type=F32).reshape(NZ, 4, TOK)
    slots = jnp.arange(CAP, dtype=jnp.int32).astype(F32)
    chosen = named[:, :, None, :] & (rank[:, :, None, :] == slots[None, None, :, None])
    sel = chosen.astype(BF16).reshape(NZ, 4 * CAP, TOK)
    table = jnp.where(chosen, weight[:, :, None, :], 0.0).reshape(NZ, 4 * CAP, TOK)
    high = table.astype(BF16)
    low = (table - high.astype(F32)).astype(BF16)

    rows = [select_rows(sel, t) for t in tok]
    own = [r[0].reshape(ROWS, HALF) for r in rows]
    sent = []
    for i, move in ((1, to_x), (2, to_y), (3, to_diagonal)):
        for h in range(2):
            sent.append(move(rows[h][i].reshape(ROWS, HALF)))
    done = ffn(pieces, sent)
    done_own = ffn(pieces, own)
    back = [
        [done_own[h]] + [move(done[2 * i + h]) for i, move in ((0, to_x), (1, to_y), (2, to_diagonal))]
        for h in range(2)
    ]
    sums = []
    for h in range(2):
        part = combine_rows(high, low, [b.reshape(NZ, CAP, HALF) for b in back[h]])
        sums.append(
            lax.psum_scatter(part.reshape(NZ * TOK, HALF), "z", scatter_dimension=0, tiled=True)
        )
    combined = jnp.where(
        d == 0, jnp.concatenate(sums, axis=1), jnp.concatenate(sums[::-1], axis=1)
    )
    return (combined, landed[0:2], landed[3:5], landed[2], landed[5])


def solution(mesh):
    fine = Mesh(mesh.devices.reshape(YL, NZ, XP, XQ, CORES, NDP), AXES)
    expert = ("yl", "z", "xp", "xq", "c")
    in_specs = (
        P(AXES, None),
        P(AXES, None),
        P(AXES, None),
        P(),
        P(None, expert, "dp"),
        P(expert, "dp"),
        P("dp", None, expert, None),
        P("dp", expert, None),
        P(None, expert, "dp"),
        P(None, expert, "dp"),
        P(expert, "dp"),
        P(expert, "dp"),
    )
    out_specs = (
        P(AXES, None),
        P(None, expert, "dp"),
        P(None, expert, "dp"),
        P(expert, "dp"),
        P(expert, "dp"),
    )
    return jax.shard_map(local, mesh=fine, in_specs=in_specs, out_specs=out_specs, check_vma=False)
```

```python
import jax
import jax.numpy as jnp
from jax import lax
from jax.experimental import pallas as pl
from jax.experimental.pallas import tpu as pltpu
from jax.sharding import Mesh
from jax.sharding import PartitionSpec as P


BETA_ONE = 0.9
BETA_TWO = 0.95
LEARNING_RATE = 0.005
EPSILON = 1e-08
CORRECT_FIRST = 1.0 / (1.0 - 0.9**10)
CORRECT_SECOND = 1.0 / (1.0 - 0.95**10)

YL, NZ, XP, XQ, CORES, NDP = 2, 8, 2, 2, 2, 2
AXES = ("yl", "z", "xp", "xq", "c", "dp")
TOK, TOP, D, HALF, HDEV, CAP = 128, 6, 2560, 1280, 192, 32
GROUPS, GROUP_ROWS = 8, 24
HID = 4 * HDEV
SWAP = [(0, 1), (1, 0)]
X_FAR = [(0, 3), (3, 0), (1, 2), (2, 1)]
DIAGONAL = [(yl * 4 + a, (1 - yl) * 4 + b) for yl in range(2) for a, b in X_FAR]

BF16, F32 = jnp.bfloat16, jnp.float32


def to_x(a):
    return lax.ppermute(a, ("xp", "xq"), X_FAR)


def to_y(a):
    return lax.ppermute(a, "yl", SWAP)


def to_diagonal(a):
    return lax.ppermute(a, ("yl", "xp", "xq"), DIAGONAL)


def exchange(a):
    return lax.all_to_all(a, ("yl", "z", "xp"), 0, 0, tiled=True)


def along_z(a, step):
    return lax.ppermute(a, "z", [(i, (i + step) % NZ) for i in range(NZ)])


def adam_kernel(d_ref, w_in, w_out, g_in, g_out, got_in, got_out, f_in, s_in, f_out, s_out, new, moments):
    for m in range(3):
        w, ga, gb, f, s = (
            (w_in[m], g_in[0, m], got_in[m], f_in[m], s_in[m])
            if m < 2
            else (w_out[...], g_out[0], got_out[...], f_out[...], s_out[...])
        )
        g = ga.astype(F32) + gb.astype(F32)
        first = BETA_ONE * f.astype(F32) + (1.0 - BETA_ONE) * g
        second = BETA_TWO * s.astype(F32) + (1.0 - BETA_TWO) * g * g
        stepped = w.astype(F32) - LEARNING_RATE * (first * CORRECT_FIRST) / (
            jnp.sqrt(second * CORRECT_SECOND) + EPSILON
        )
        new[m] = stepped.astype(BF16)
        for i, moment in enumerate((first, second)):
            for h in range(2):
                moments[i, 0, h, m * GROUP_ROWS : (m + 1) * GROUP_ROWS] = moment[
                    :, h * 640 : (h + 1) * 640
                ].astype(BF16)


def adam(d, w_in, w_out, g_in, g_out, got_in, got_out, f_in, s_in, f_out, s_out):
    block = GROUP_ROWS
    three = pl.BlockSpec((2, block, HALF), lambda i, d: (0, i, 0))
    two = pl.BlockSpec((block, HALF), lambda i, d: (i, 0))
    return pl.pallas_call(
        adam_kernel,
        grid_spec=pltpu.PrefetchScalarGridSpec(
            num_scalar_prefetch=1,
            grid=(GROUPS,),
            in_specs=[
                three,
                two,
                pl.BlockSpec((1, 2, block, HALF), lambda i, d: (0, 0, i, d[0])),
                pl.BlockSpec((1, block, HALF), lambda i, d: (0, i, d[0])),
                three,
                two,
                three,
                three,
                two,
                two,
            ],
            out_specs=[
                pl.BlockSpec((3, block, HALF), lambda i, d: (0, i, 0)),
                pl.BlockSpec((2, 1, 2, 3 * block, 640), lambda i, d: (0, i, 0, 0, 0)),
            ],
        ),
        out_shape=[
            jax.ShapeDtypeStruct((3, HDEV, HALF), BF16),
            jax.ShapeDtypeStruct((2, GROUPS, 2, 3 * block, 640), BF16),
        ],
        name="adam",
    )(d, w_in, w_out, g_in, g_out, got_in, got_out, f_in, s_in, f_out, s_out)


def unpack_kernel(landed, f_in, s_in, f_out, s_out):
    for i, (inward, outward) in enumerate(((f_in, f_out), (s_in, s_out))):
        for m in range(3):
            for h in range(2):
                part = landed[i, 0, h, m * GROUP_ROWS : (m + 1) * GROUP_ROWS]
                if m < 2:
                    inward[m, :, h * 640 : (h + 1) * 640] = part
                else:
                    outward[:, h * 640 : (h + 1) * 640] = part


def unpack(landed):
    block = GROUP_ROWS
    three = pl.BlockSpec((2, block, HALF), lambda i: (0, i, 0))
    two = pl.BlockSpec((block, HALF), lambda i: (i, 0))
    inward = jax.ShapeDtypeStruct((2, HDEV, HALF), BF16)
    outward = jax.ShapeDtypeStruct((HDEV, HALF), BF16)
    return pl.pallas_call(
        unpack_kernel,
        grid=(GROUPS,),
        in_specs=[pl.BlockSpec((2, 1, 2, 3 * block, 640), lambda i: (0, i, 0, 0, 0))],
        out_specs=[three, three, two, two],
        out_shape=[inward, inward, outward, outward],
        name="unpack",
    )(landed)


def select_kernel(count, experts, *refs):
    messages, outs, (high, low) = refs[:count], refs[count : count + 4], refs[count + 4 :]
    lane = lax.broadcasted_iota(jnp.int32, (TOK, 4 * CAP), 1)
    row = lax.broadcasted_iota(jnp.int32, (TOK, TOK), 0)
    column = lax.broadcasted_iota(jnp.int32, (TOK, TOK), 1)
    before = jnp.where(column < row, 1.0, 0.0).astype(BF16)
    block, slot = lane // CAP, (lane % CAP).astype(F32)
    mine = jnp.where(
        block == 0, experts[0], jnp.where(block == 1, experts[1], jnp.where(block == 2, experts[2], experts[3]))
    ).astype(F32)
    for i, message in enumerate(messages):
        listing = message[:, D:].astype(F32)
        named = jnp.zeros((TOK, 4 * CAP), F32)
        weight = jnp.zeros((TOK, 4 * CAP), F32)
        for k in range(TOP):
            hit = listing[:, k : k + 1] == mine
            value = listing[:, 8 + k : 9 + k] + listing[:, 16 + k : 17 + k]
            named = jnp.where(hit, 1.0, named)
            weight = jnp.where(hit, value, weight)
        rank = jnp.dot(before, named.astype(BF16), preferred_element_type=F32)
        chosen = jnp.where(rank == slot, named, 0.0)
        table = chosen * weight
        top = table.astype(BF16)
        high[i] = top
        low[i] = (table - top.astype(F32)).astype(BF16)
        rows = lax.dot_general(
            chosen.astype(BF16), message[:, :D], (((0,), (0,)), ((), ())), preferred_element_type=F32
        ).astype(BF16)
        for b, out in enumerate(outs):
            out[i * CAP : (i + 1) * CAP] = rows[b * CAP : (b + 1) * CAP]


def select_rows(experts, messages):
    count = len(messages)
    here = pl.BlockSpec(memory_space=pltpu.VMEM)
    outs = pl.pallas_call(
        lambda *refs: select_kernel(count, *refs),
        in_specs=[pl.BlockSpec(memory_space=pltpu.SMEM)] + [here] * count,
        out_specs=[here] * 6,
        out_shape=[jax.ShapeDtypeStruct((count * CAP, D), BF16)] * 4
        + [jax.ShapeDtypeStruct((count, TOK, 4 * CAP), BF16)] * 2,
    )(experts, *messages)
    return outs[:4], outs[4:]


def combine_kernel(count, high, low, *refs):
    parts, outs = refs[:4], refs[4:]
    for i in range(count):
        rows = jnp.concatenate([part[i * CAP : (i + 1) * CAP] for part in parts], axis=0)
        total = jnp.dot(high[i], rows, preferred_element_type=F32)
        total = total + jnp.dot(low[i], rows, preferred_element_type=F32)
        outs[i][...] = total.astype(BF16)


def combine_rows(tables, parts):
    count = tables[0].shape[0]
    here = pl.BlockSpec(memory_space=pltpu.VMEM)
    return pl.pallas_call(
        lambda *refs: combine_kernel(count, *refs),
        in_specs=[here] * 6,
        out_specs=[here] * count,
        out_shape=[jax.ShapeDtypeStruct((TOK, D), BF16)] * count,
    )(*tables, *parts)


def ffn_kernel(share, *refs):
    pieces, rows, outs = refs[:8], refs[8:12], refs[12:16]
    weights, held, result, weight_sem, row_sem, out_sem = refs[16:]
    copies = []
    for h in range(2):
        for m in range(3):
            for q in range(4):
                copies.append(
                    pltpu.make_async_copy(
                        pieces[2 * q + h].at[m], weights.at[h, m, pl.ds(q * HDEV, HDEV)], weight_sem.at[q, h, m]
                    )
                )
    for i in range(4):
        copies.append(pltpu.make_async_copy(rows[i], held.at[pl.ds(i * share, share)], row_sem.at[i]))
    for copy in copies:
        copy.start()
    for copy in copies:
        copy.wait()
    nt = (((1,), (1,)), ((), ()))
    step = 2 * share

    def one_block(i, carry):
        begin = pl.multiple_of(i * step, step)
        x0, x1 = held[pl.ds(begin, step), :HALF], held[pl.ds(begin, step), HALF:]

        def project(m):
            return lax.dot_general(x0, weights[0, m], nt, preferred_element_type=F32) + lax.dot_general(
                x1, weights[1, m], nt, preferred_element_type=F32
            )

        hidden = (jax.nn.silu(project(0)) * project(1)).astype(BF16)
        for h in range(2):
            result[pl.ds(begin, step), h * HALF : (h + 1) * HALF] = jnp.dot(
                hidden, weights[h, 2], preferred_element_type=F32
            ).astype(BF16)
        return carry

    lax.fori_loop(0, 2, one_block, 0)
    copies = [
        pltpu.make_async_copy(result.at[pl.ds(i * share, share)], outs[i], out_sem.at[i]) for i in range(4)
    ]
    for copy in copies:
        copy.start()
    for copy in copies:
        copy.wait()


def ffn(pieces, rows):
    share = rows[0].shape[0]
    anywhere = pl.BlockSpec(memory_space=pl.ANY)
    return pl.pallas_call(
        lambda *refs: ffn_kernel(share, *refs),
        in_specs=[anywhere] * 12,
        out_specs=[anywhere] * 4,
        out_shape=[jax.ShapeDtypeStruct((share, D), BF16)] * 4,
        scratch_shapes=[
            pltpu.VMEM((2, 3, HID, HALF), BF16),
            pltpu.VMEM((4 * share, D), BF16),
            pltpu.VMEM((4 * share, D), BF16),
            pltpu.SemaphoreType.DMA((4, 2, 3)),
            pltpu.SemaphoreType.DMA((4,)),
            pltpu.SemaphoreType.DMA((4,)),
        ],
    )(*pieces, *rows)


def halves(a, d, axis):
    left, right = jnp.split(a, 2, axis=axis)
    return jnp.where(d == 0, left, right), jnp.where(d == 0, right, left)


def plus(a, *others):
    total = a.astype(F32)
    for b in others:
        total = total + b.astype(F32)
    return total.astype(BF16)


MOVES = ((to_y, "y"), (to_diagonal, "d"), (to_x, "x"))


def layer(tokens, routes, combine_weight, owner_plan, w_in, w_out, grad_in, grad_out, first_in, second_in, first_out, second_out):
    d = lax.axis_index("dp")
    yl, z, xp = lax.axis_index("yl"), lax.axis_index("z"), lax.axis_index("xp")
    experts = jnp.stack(
        [a * 16 + z * 2 + b for a, b in ((yl, xp), (yl, 1 - xp), (1 - yl, xp), (1 - yl, 1 - xp))]
    ).astype(jnp.int32)

    def permute(a, axis):
        return lax.ppermute(a, axis, SWAP)

    def spread_out(rows):
        got = {"o": rows[0]}
        for (move, tag), r in zip(MOVES, (rows[2], rows[3], rows[1])):
            got[tag] = move(r)
        return [got["o"], got["x"], got["y"], got["d"]]

    high = combine_weight.astype(BF16)
    low = (combine_weight - high.astype(F32)).astype(BF16)
    gap = jnp.zeros((TOK, 2), BF16)
    mine = jnp.concatenate(
        [*halves(tokens, d, 1), routes.astype(BF16), gap, high, gap, low, jnp.zeros((TOK, 106), BF16)], axis=1
    )
    up, down = [mine], [mine]
    for _ in range(3):
        up.append(along_z(up[-1], 1))
        down.append(along_z(down[-1], -1))
    across = jnp.concatenate([along_z(up[3][: TOK // 2], 1), along_z(down[3][TOK // 2 :], -1)], axis=0)

    got_in = permute(halves(grad_in[0], d, 2)[1], "dp")
    got_out = permute(halves(grad_out[0], d, 1)[1], "dp")
    new, moments = adam(
        d.reshape(1), w_in, w_out, grad_in, grad_out, got_in, got_out, first_in, second_in, first_out, second_out
    )
    other = permute(new, "dp")
    far_new = permute(new, "xq")
    core_new = permute(new, "c")
    far_other = permute(other, "xq")
    core_other = permute(other, "c")
    core_far_new = permute(far_new, "c")
    core_far_other = permute(far_other, "c")
    pieces = [new, other, far_new, far_other, core_new, core_other, core_far_new, core_far_other]

    near_rows, near_tables = select_rows(experts, [mine, up[1], down[1], up[2], down[2]])
    near_got = spread_out(near_rows)
    far_rows, far_tables = select_rows(experts, [up[3], down[3], across])
    far_got = spread_out(far_rows)

    spread = exchange(moments.reshape(32, 72, 640))
    picked = spread.at[owner_plan].get(mode="promise_in_bounds")
    landed = exchange(picked)
    next_moments = unpack(landed.reshape(2, GROUPS, 2, 72, 640))

    far_done = ffn(pieces, far_got)
    far_back = spread_out(far_done)
    near_done = ffn(pieces, near_got)
    near_back = spread_out(near_done)

    below3, above3, opposite = combine_rows(far_tables, far_back)
    here, below1, above1, below2, above2 = combine_rows(near_tables, near_back)
    rest = TOK // 2
    rising = along_z(opposite[:rest], 1)
    falling = along_z(opposite[rest:], -1)
    rising = jnp.concatenate([plus(above3[:rest], rising), above3[rest:]], axis=0)
    falling = jnp.concatenate([below3[:rest], plus(below3[rest:], falling)], axis=0)
    rising = along_z(rising, 1)
    falling = along_z(falling, -1)
    rising = along_z(plus(above2, rising), 1)
    falling = along_z(plus(below2, falling), -1)
    rising = along_z(plus(above1, rising), 1)
    falling = along_z(plus(below1, falling), -1)
    total = plus(here, rising, falling)
    combined = jnp.where(d == 0, total, jnp.concatenate([total[:, HALF:], total[:, :HALF]], axis=1))
    return (combined, *next_moments)


def solution(mesh):
    fine = Mesh(mesh.devices.reshape(YL, NZ, XP, XQ, CORES, NDP), AXES)
    expert = ("yl", "z", "xp", "xq", "c")
    in_specs = (
        P(AXES, None),
        P(AXES, None),
        P(AXES, None),
        P(),
        P(None, expert, "dp"),
        P(expert, "dp"),
        P("dp", None, expert, None),
        P("dp", expert, None),
        P(None, expert, "dp"),
        P(None, expert, "dp"),
        P(expert, "dp"),
        P(expert, "dp"),
    )
    out_specs = (
        P(AXES, None),
        P(None, expert, "dp"),
        P(None, expert, "dp"),
        P(expert, "dp"),
        P(expert, "dp"),
    )
    return jax.shard_map(layer, mesh=fine, in_specs=in_specs, out_specs=out_specs, check_vma=False)
```

```python
import jax
import jax.numpy as jnp
from jax import lax
from jax.experimental import pallas as pl
from jax.experimental.pallas import tpu as pltpu
from jax.sharding import Mesh
from jax.sharding import PartitionSpec as P


BETA_ONE = 0.9
BETA_TWO = 0.95
LEARNING_RATE = 0.005
EPSILON = 1e-08
CORRECT_FIRST = 1.0 / (1.0 - 0.9**10)
CORRECT_SECOND = 1.0 / (1.0 - 0.95**10)

YL, NZ, XP, XQ, CORES, NDP = 2, 8, 2, 2, 2, 2
AXES = ("yl", "z", "xp", "xq", "c", "dp")
TOK, TOP, D, HALF, HDEV, CAP = 128, 6, 2560, 1280, 192, 32
GROUPS, GROUP_ROWS = 8, 24
HID = 4 * HDEV
SIZES = (CAP, CAP, CAP // 2, CAP // 2, CAP // 2, CAP // 2)
SWAPPED = (3, 5)
SWAP = [(0, 1), (1, 0)]
X_FAR = [(0, 3), (3, 0), (1, 2), (2, 1)]
DIAGONAL = [(yl * 4 + a, (1 - yl) * 4 + b) for yl in range(2) for a, b in X_FAR]
OUTER = [(0, 3), (3, 0), (1, 2), (2, 1)]
OUTER_DIAGONAL = [(a * 2 + dp, b * 2 + 1 - dp) for a, b in DIAGONAL for dp in range(2)]

BF16, F32 = jnp.bfloat16, jnp.float32


def to_x(a):
    return lax.ppermute(a, ("xp", "xq"), X_FAR)


def to_y(a):
    return lax.ppermute(a, "yl", SWAP)


def to_diagonal(a):
    return lax.ppermute(a, ("yl", "xp", "xq"), DIAGONAL)


def to_outer_y(a):
    return lax.ppermute(a, ("yl", "dp"), OUTER)


def to_outer_diagonal(a):
    return lax.ppermute(a, ("yl", "xp", "xq", "dp"), OUTER_DIAGONAL)


def exchange(a):
    return lax.all_to_all(a, ("yl", "z", "xp"), 0, 0, tiled=True)


def along_z(a, step):
    return lax.ppermute(a, "z", [(i, (i + step) % NZ) for i in range(NZ)])


def adam_kernel(d_ref, w_in, w_out, g_in, g_out, got_in, got_out, f_in, s_in, f_out, s_out, new, moments):
    for m in range(3):
        w, ga, gb, f, s = (
            (w_in[m], g_in[0, m], got_in[m], f_in[m], s_in[m])
            if m < 2
            else (w_out[...], g_out[0], got_out[...], f_out[...], s_out[...])
        )
        g = ga.astype(F32) + gb.astype(F32)
        first = BETA_ONE * f.astype(F32) + (1.0 - BETA_ONE) * g
        second = BETA_TWO * s.astype(F32) + (1.0 - BETA_TWO) * g * g
        stepped = w.astype(F32) - LEARNING_RATE * (first * CORRECT_FIRST) / (
            jnp.sqrt(second * CORRECT_SECOND) + EPSILON
        )
        new[m] = stepped.astype(BF16)
        for i, moment in enumerate((first, second)):
            for h in range(2):
                moments[i, 0, h, m * GROUP_ROWS : (m + 1) * GROUP_ROWS] = moment[
                    :, h * 640 : (h + 1) * 640
                ].astype(BF16)


def adam(d, w_in, w_out, g_in, g_out, got_in, got_out, f_in, s_in, f_out, s_out):
    block = GROUP_ROWS
    three = pl.BlockSpec((2, block, HALF), lambda i, d: (0, i, 0))
    two = pl.BlockSpec((block, HALF), lambda i, d: (i, 0))
    return pl.pallas_call(
        adam_kernel,
        grid_spec=pltpu.PrefetchScalarGridSpec(
            num_scalar_prefetch=1,
            grid=(GROUPS,),
            in_specs=[
                three,
                two,
                pl.BlockSpec((1, 2, block, HALF), lambda i, d: (0, 0, i, d[0])),
                pl.BlockSpec((1, block, HALF), lambda i, d: (0, i, d[0])),
                three,
                two,
                three,
                three,
                two,
                two,
            ],
            out_specs=[
                pl.BlockSpec((3, block, HALF), lambda i, d: (0, i, 0)),
                pl.BlockSpec((2, 1, 2, 3 * block, 640), lambda i, d: (0, i, 0, 0, 0)),
            ],
        ),
        out_shape=[
            jax.ShapeDtypeStruct((3, HDEV, HALF), BF16),
            jax.ShapeDtypeStruct((2, GROUPS, 2, 3 * block, 640), BF16),
        ],
        name="adam",
    )(d, w_in, w_out, g_in, g_out, got_in, got_out, f_in, s_in, f_out, s_out)


def unpack_kernel(landed, f_in, s_in, f_out, s_out):
    for i, (inward, outward) in enumerate(((f_in, f_out), (s_in, s_out))):
        for m in range(3):
            for h in range(2):
                part = landed[i, 0, h, m * GROUP_ROWS : (m + 1) * GROUP_ROWS]
                if m < 2:
                    inward[m, :, h * 640 : (h + 1) * 640] = part
                else:
                    outward[:, h * 640 : (h + 1) * 640] = part


def unpack(landed):
    block = GROUP_ROWS
    three = pl.BlockSpec((2, block, HALF), lambda i: (0, i, 0))
    two = pl.BlockSpec((block, HALF), lambda i: (i, 0))
    inward = jax.ShapeDtypeStruct((2, HDEV, HALF), BF16)
    outward = jax.ShapeDtypeStruct((HDEV, HALF), BF16)
    return pl.pallas_call(
        unpack_kernel,
        grid=(GROUPS,),
        in_specs=[pl.BlockSpec((2, 1, 2, 3 * block, 640), lambda i: (0, i, 0, 0, 0))],
        out_specs=[three, three, two, two],
        out_shape=[inward, inward, outward, outward],
        name="unpack",
    )(landed)


def select_kernel(count, experts, *refs):
    messages, outs, (high, low) = refs[:count], refs[count : count + 6], refs[count + 6 :]
    lane = lax.broadcasted_iota(jnp.int32, (TOK, 4 * CAP), 1)
    row = lax.broadcasted_iota(jnp.int32, (TOK, TOK), 0)
    column = lax.broadcasted_iota(jnp.int32, (TOK, TOK), 1)
    before = jnp.where(column < row, 1.0, 0.0).astype(BF16)
    block, slot = lane // CAP, (lane % CAP).astype(F32)
    mine = jnp.where(
        block == 0, experts[0], jnp.where(block == 1, experts[1], jnp.where(block == 2, experts[2], experts[3]))
    ).astype(F32)
    for i, message in enumerate(messages):
        listing = message[:, D:].astype(F32)
        named = jnp.zeros((TOK, 4 * CAP), F32)
        weight = jnp.zeros((TOK, 4 * CAP), F32)
        for k in range(TOP):
            hit = listing[:, k : k + 1] == mine
            value = listing[:, 8 + k : 9 + k] + listing[:, 16 + k : 17 + k]
            named = jnp.where(hit, 1.0, named)
            weight = jnp.where(hit, value, weight)
        rank = jnp.dot(before, named.astype(BF16), preferred_element_type=F32)
        chosen = jnp.where(rank == slot, named, 0.0)
        table = chosen * weight
        top = table.astype(BF16)
        high[i] = top
        low[i] = (table - top.astype(F32)).astype(BF16)
        rows = lax.dot_general(
            chosen.astype(BF16), message[:, :D], (((0,), (0,)), ((), ())), preferred_element_type=F32
        ).astype(BF16)
        begin = 0
        for out, size in zip(outs, SIZES):
            out[i * size : (i + 1) * size] = rows[begin : begin + size]
            begin += size


def select_rows(experts, messages):
    count = len(messages)
    here = pl.BlockSpec(memory_space=pltpu.VMEM)
    outs = pl.pallas_call(
        lambda *refs: select_kernel(count, *refs),
        in_specs=[pl.BlockSpec(memory_space=pltpu.SMEM)] + [here] * count,
        out_specs=[here] * 8,
        out_shape=[jax.ShapeDtypeStruct((count * size, D), BF16) for size in SIZES]
        + [jax.ShapeDtypeStruct((count, TOK, 4 * CAP), BF16)] * 2,
    )(experts, *messages)
    return outs[:6], outs[6:]


def combine_kernel(count, high, low, *refs):
    parts, outs = refs[:6], refs[6:]
    for i in range(count):
        rows = jnp.concatenate(
            [part[i * size : (i + 1) * size] for part, size in zip(parts, SIZES)], axis=0
        )
        total = jnp.dot(high[i], rows, preferred_element_type=F32)
        total = total + jnp.dot(low[i], rows, preferred_element_type=F32)
        outs[i][...] = total.astype(BF16)


def combine_rows(tables, parts):
    count = tables[0].shape[0]
    here = pl.BlockSpec(memory_space=pltpu.VMEM)
    return pl.pallas_call(
        lambda *refs: combine_kernel(count, *refs),
        in_specs=[here] * 8,
        out_specs=[here] * count,
        out_shape=[jax.ShapeDtypeStruct((TOK, D), BF16)] * count,
    )(*tables, *parts)


def ffn_kernel(count, *refs):
    new, far_new, core_new, core_far_new = refs[:4]
    others = refs[4:16]
    rows, outs = refs[16:22], refs[22:28]
    weights, held, result, weight_sem, row_sem, out_sem = refs[28:]
    share = 4 * CAP * count
    step = share // 2

    def moved(arrays, buffer, sem, inward):
        copies, begin = [], 0
        for i, (array, size) in enumerate(zip(arrays, SIZES)):
            place = pl.ds(begin, count * size)
            for h in range(2):
                far = array.at[:, pl.ds(h * HALF, HALF)]
                near = buffer.at[place, pl.ds((1 - h if i in SWAPPED else h) * HALF, HALF)]
                copies.append(pltpu.make_async_copy(*((far, near) if inward else (near, far)), sem.at[i, h]))
            begin += count * size
        return copies

    copies = []
    for m in range(3):
        for q, piece in enumerate((new, far_new, core_new, core_far_new)):
            place = pl.ds(q * HDEV, HDEV)
            copies.append(pltpu.make_async_copy(piece.at[m], weights.at[0, m, place], weight_sem.at[q, 0, m]))
            copies.append(
                pltpu.make_async_copy(others[3 * q + m], weights.at[1, m, place], weight_sem.at[q, 1, m])
            )
    copies += moved(rows, held, row_sem, True)
    for copy in copies:
        copy.start()
    for copy in copies:
        copy.wait()
    nt = (((1,), (1,)), ((), ()))

    def one_block(i, carry):
        begin = pl.multiple_of(i * step, step)
        x0, x1 = held[pl.ds(begin, step), :HALF], held[pl.ds(begin, step), HALF:]

        def project(m):
            return lax.dot_general(x0, weights[0, m], nt, preferred_element_type=F32) + lax.dot_general(
                x1, weights[1, m], nt, preferred_element_type=F32
            )

        hidden = (jax.nn.silu(project(0)) * project(1)).astype(BF16)
        for h in range(2):
            result[pl.ds(begin, step), h * HALF : (h + 1) * HALF] = jnp.dot(
                hidden, weights[h, 2], preferred_element_type=F32
            ).astype(BF16)
        return carry

    lax.fori_loop(0, 2, one_block, 0)
    copies = moved(outs, result, out_sem, False)
    for copy in copies:
        copy.start()
    for copy in copies:
        copy.wait()


def ffn(pieces, rows):
    count = rows[0].shape[0] // CAP
    share = 4 * CAP * count
    anywhere = pl.BlockSpec(memory_space=pl.ANY)
    return pl.pallas_call(
        lambda *refs: ffn_kernel(count, *refs),
        in_specs=[anywhere] * 22,
        out_specs=[anywhere] * 6,
        out_shape=[jax.ShapeDtypeStruct((count * size, D), BF16) for size in SIZES],
        scratch_shapes=[
            pltpu.VMEM((2, 3, HID, HALF), BF16),
            pltpu.VMEM((share, D), BF16),
            pltpu.VMEM((share, D), BF16),
            pltpu.SemaphoreType.DMA((4, 2, 3)),
            pltpu.SemaphoreType.DMA((6, 2)),
            pltpu.SemaphoreType.DMA((6, 2)),
        ],
    )(*pieces, *rows)


def halves(a, d, axis):
    left, right = jnp.split(a, 2, axis=axis)
    return jnp.where(d == 0, left, right), jnp.where(d == 0, right, left)


def plus(a, *others):
    total = a.astype(F32)
    for b in others:
        total = total + b.astype(F32)
    return total.astype(BF16)


MOVES = ((4, to_diagonal), (5, to_outer_diagonal), (2, to_y), (3, to_outer_y), (1, to_x))


def layer(tokens, routes, combine_weight, owner_plan, w_in, w_out, grad_in, grad_out, first_in, second_in, first_out, second_out):
    d = lax.axis_index("dp")
    yl, z, xp = lax.axis_index("yl"), lax.axis_index("z"), lax.axis_index("xp")
    experts = jnp.stack(
        [a * 16 + z * 2 + b for a, b in ((yl, xp), (yl, 1 - xp), (1 - yl, xp), (1 - yl, 1 - xp))]
    ).astype(jnp.int32)

    def permute(a, axis):
        return lax.ppermute(a, axis, SWAP)

    def spread_out(rows):
        got = list(rows)
        for i, move in MOVES:
            got[i] = move(rows[i])
        return got

    high = combine_weight.astype(BF16)
    low = (combine_weight - high.astype(F32)).astype(BF16)
    gap = jnp.zeros((TOK, 2), BF16)
    mine = jnp.concatenate(
        [*halves(tokens, d, 1), routes.astype(BF16), gap, high, gap, low, jnp.zeros((TOK, 106), BF16)], axis=1
    )
    up, down = [mine], [mine]
    for _ in range(3):
        up.append(along_z(up[-1], 1))
        down.append(along_z(down[-1], -1))
    across = jnp.concatenate([along_z(up[3][: TOK // 2], 1), along_z(down[3][TOK // 2 :], -1)], axis=0)

    got_in = permute(halves(grad_in[0], d, 2)[1], "dp")
    got_out = permute(halves(grad_out[0], d, 1)[1], "dp")
    new, moments = adam(
        d.reshape(1), w_in, w_out, grad_in, grad_out, got_in, got_out, first_in, second_in, first_out, second_out
    )

    def by_matrix(arrays, axis):
        return [permute(a, axis) for a in arrays]

    other = by_matrix([new[m] for m in range(3)], "dp")
    far_new = permute(new, "xq")
    core_new = permute(new, "c")
    far_other = by_matrix(other, "xq")
    core_other = by_matrix(other, "c")
    core_far_new = permute(far_new, "c")
    core_far_other = by_matrix(far_other, "c")
    pieces = [new, far_new, core_new, core_far_new, *other, *far_other, *core_other, *core_far_other]

    near_rows, near_tables = select_rows(experts, [mine, up[1], down[1], up[2], down[2]])
    near_got = spread_out(near_rows)
    far_rows, far_tables = select_rows(experts, [up[3], down[3], across])
    far_got = spread_out(far_rows)

    spread = exchange(moments.reshape(32, 72, 640))
    picked = spread.at[owner_plan].get(mode="promise_in_bounds")
    landed = exchange(picked)
    next_moments = unpack(landed.reshape(2, GROUPS, 2, 72, 640))

    far_done = ffn(pieces, far_got)
    far_back = spread_out(far_done)
    near_done = ffn(pieces, near_got)
    near_back = spread_out(near_done)

    below3, above3, opposite = combine_rows(far_tables, far_back)
    here, below1, above1, below2, above2 = combine_rows(near_tables, near_back)
    rest = TOK // 2
    rising = along_z(opposite[:rest], 1)
    falling = along_z(opposite[rest:], -1)
    rising = jnp.concatenate([plus(above3[:rest], rising), above3[rest:]], axis=0)
    falling = jnp.concatenate([below3[:rest], plus(below3[rest:], falling)], axis=0)
    rising = along_z(rising, 1)
    falling = along_z(falling, -1)
    rising = along_z(plus(above2, rising), 1)
    falling = along_z(plus(below2, falling), -1)
    rising = along_z(plus(above1, rising), 1)
    falling = along_z(plus(below1, falling), -1)
    total = plus(here, rising, falling)
    combined = jnp.where(d == 0, total, jnp.concatenate([total[:, HALF:], total[:, :HALF]], axis=1))
    return (combined, *next_moments)


def solution(mesh):
    fine = Mesh(mesh.devices.reshape(YL, NZ, XP, XQ, CORES, NDP), AXES)
    expert = ("yl", "z", "xp", "xq", "c")
    in_specs = (
        P(AXES, None),
        P(AXES, None),
        P(AXES, None),
        P(),
        P(None, expert, "dp"),
        P(expert, "dp"),
        P("dp", None, expert, None),
        P("dp", expert, None),
        P(None, expert, "dp"),
        P(None, expert, "dp"),
        P(expert, "dp"),
        P(expert, "dp"),
    )
    out_specs = (
        P(AXES, None),
        P(None, expert, "dp"),
        P(None, expert, "dp"),
        P(expert, "dp"),
        P(expert, "dp"),
    )
    return jax.shard_map(layer, mesh=fine, in_specs=in_specs, out_specs=out_specs, check_vma=False)
```

```python
import jax
import jax.numpy as jnp
from jax import lax
from jax.experimental import pallas as pl
from jax.experimental.pallas import tpu as pltpu
from jax.sharding import Mesh
from jax.sharding import PartitionSpec as P


BETA_ONE = 0.9
BETA_TWO = 0.95
LEARNING_RATE = 0.005
EPSILON = 1e-08
CORRECT_FIRST = 1.0 / (1.0 - 0.9**10)
CORRECT_SECOND = 1.0 / (1.0 - 0.95**10)

YL, NZ, XP, XQ, CORES, NDP = 2, 8, 2, 2, 2, 2
AXES = ("yl", "z", "xp", "xq", "c", "dp")
TOK, TOP, D, HALF, HDEV, CAP = 128, 6, 2560, 1280, 192, 32
GROUPS, GROUP_ROWS = 8, 24
HID = 4 * HDEV
SIZES = (CAP, CAP, CAP // 2, CAP // 2, CAP // 2, CAP // 2)
SWAPPED = (3, 5)
SWAP = [(0, 1), (1, 0)]
X_FAR = [(0, 3), (3, 0), (1, 2), (2, 1)]
DIAGONAL = [(yl * 4 + a, (1 - yl) * 4 + b) for yl in range(2) for a, b in X_FAR]
OUTER = [(0, 3), (3, 0), (1, 2), (2, 1)]
OUTER_DIAGONAL = [(a * 2 + dp, b * 2 + 1 - dp) for a, b in DIAGONAL for dp in range(2)]

BF16, F32 = jnp.bfloat16, jnp.float32


def to_x(a):
    return lax.ppermute(a, ("xp", "xq"), X_FAR)


def to_y(a):
    return lax.ppermute(a, "yl", SWAP)


def to_diagonal(a):
    return lax.ppermute(a, ("yl", "xp", "xq"), DIAGONAL)


def to_outer_y(a):
    return lax.ppermute(a, ("yl", "dp"), OUTER)


def to_outer_diagonal(a):
    return lax.ppermute(a, ("yl", "xp", "xq", "dp"), OUTER_DIAGONAL)


def exchange(a, axes):
    return lax.all_to_all(a, axes, 0, 0, tiled=True)


def along_z(a, step):
    return lax.ppermute(a, "z", [(i, (i + step) % NZ) for i in range(NZ)])


def adam_kernel(d_ref, w_in, w_out, g_in, g_out, got_in, got_out, f_in, s_in, f_out, s_out, new, moments, *apart):
    for m in range(3):
        w, ga, gb, f, s = (
            (w_in[m], g_in[0, m], got_in[m], f_in[m], s_in[m])
            if m < 2
            else (w_out[...], g_out[0], got_out[...], f_out[...], s_out[...])
        )
        g = ga.astype(F32) + gb.astype(F32)
        first = BETA_ONE * f.astype(F32) + (1.0 - BETA_ONE) * g
        second = BETA_TWO * s.astype(F32) + (1.0 - BETA_TWO) * g * g
        stepped = w.astype(F32) - LEARNING_RATE * (first * CORRECT_FIRST) / (
            jnp.sqrt(second * CORRECT_SECOND) + EPSILON
        )
        new[m] = apart[m][...] = stepped.astype(BF16)
        for i, moment in enumerate((first, second)):
            for h in range(2):
                moments[i, h, 0, m * GROUP_ROWS : (m + 1) * GROUP_ROWS] = moment[
                    :, h * 640 : (h + 1) * 640
                ].astype(BF16)


def adam(d, w_in, w_out, g_in, g_out, got_in, got_out, f_in, s_in, f_out, s_out):
    block = GROUP_ROWS
    three = pl.BlockSpec((2, block, HALF), lambda i, d: (0, i, 0))
    two = pl.BlockSpec((block, HALF), lambda i, d: (i, 0))
    return pl.pallas_call(
        adam_kernel,
        grid_spec=pltpu.PrefetchScalarGridSpec(
            num_scalar_prefetch=1,
            grid=(GROUPS,),
            in_specs=[
                three,
                two,
                pl.BlockSpec((1, 2, block, HALF), lambda i, d: (0, 0, i, d[0])),
                pl.BlockSpec((1, block, HALF), lambda i, d: (0, i, d[0])),
                three,
                two,
                three,
                three,
                two,
                two,
            ],
            out_specs=[
                pl.BlockSpec((3, block, HALF), lambda i, d: (0, i, 0)),
                pl.BlockSpec((2, 2, 1, 3 * block, 640), lambda i, d: (0, 0, i, 0, 0)),
                two,
                two,
                two,
            ],
        ),
        out_shape=[
            jax.ShapeDtypeStruct((3, HDEV, HALF), BF16),
            jax.ShapeDtypeStruct((2, 2, GROUPS, 3 * block, 640), BF16),
        ]
        + [jax.ShapeDtypeStruct((HDEV, HALF), BF16)] * 3,
        name="adam",
    )(d, w_in, w_out, g_in, g_out, got_in, got_out, f_in, s_in, f_out, s_out)


def unpack_kernel(landed, f_in, s_in, f_out, s_out):
    for i, (inward, outward) in enumerate(((f_in, f_out), (s_in, s_out))):
        for m in range(3):
            for h in range(2):
                part = landed[i, h, 0, m * GROUP_ROWS : (m + 1) * GROUP_ROWS]
                if m < 2:
                    inward[m, :, h * 640 : (h + 1) * 640] = part
                else:
                    outward[:, h * 640 : (h + 1) * 640] = part


def unpack(landed):
    block = GROUP_ROWS
    three = pl.BlockSpec((2, block, HALF), lambda i: (0, i, 0))
    two = pl.BlockSpec((block, HALF), lambda i: (i, 0))
    inward = jax.ShapeDtypeStruct((2, HDEV, HALF), BF16)
    outward = jax.ShapeDtypeStruct((HDEV, HALF), BF16)
    return pl.pallas_call(
        unpack_kernel,
        grid=(GROUPS,),
        in_specs=[pl.BlockSpec((2, 2, 1, 3 * block, 640), lambda i: (0, 0, i, 0, 0))],
        out_specs=[three, three, two, two],
        out_shape=[inward, inward, outward, outward],
        name="unpack",
    )(landed)


def select_kernel(count, experts, *refs):
    messages, outs, (high, low) = refs[:count], refs[count : count + 6], refs[count + 6 :]
    lane = lax.broadcasted_iota(jnp.int32, (TOK, 4 * CAP), 1)
    row = lax.broadcasted_iota(jnp.int32, (TOK, TOK), 0)
    column = lax.broadcasted_iota(jnp.int32, (TOK, TOK), 1)
    before = jnp.where(column < row, 1.0, 0.0).astype(BF16)
    block, slot = lane // CAP, (lane % CAP).astype(F32)
    mine = jnp.where(
        block == 0, experts[0], jnp.where(block == 1, experts[1], jnp.where(block == 2, experts[2], experts[3]))
    ).astype(F32)
    for i, message in enumerate(messages):
        listing = message[:, D:].astype(F32)
        named = jnp.zeros((TOK, 4 * CAP), F32)
        weight = jnp.zeros((TOK, 4 * CAP), F32)
        for k in range(TOP):
            hit = listing[:, k : k + 1] == mine
            value = listing[:, 8 + k : 9 + k] + listing[:, 16 + k : 17 + k]
            named = jnp.where(hit, 1.0, named)
            weight = jnp.where(hit, value, weight)
        rank = jnp.dot(before, named.astype(BF16), preferred_element_type=F32)
        chosen = jnp.where(rank == slot, named, 0.0)
        table = chosen * weight
        top = table.astype(BF16)
        high[i] = top
        low[i] = (table - top.astype(F32)).astype(BF16)
        rows = lax.dot_general(
            chosen.astype(BF16), message[:, :D], (((0,), (0,)), ((), ())), preferred_element_type=F32
        ).astype(BF16)
        begin = 0
        for out, size in zip(outs, SIZES):
            out[i * size : (i + 1) * size] = rows[begin : begin + size]
            begin += size


def select_rows(experts, messages):
    count = len(messages)
    here = pl.BlockSpec(memory_space=pltpu.VMEM)
    outs = pl.pallas_call(
        lambda *refs: select_kernel(count, *refs),
        in_specs=[pl.BlockSpec(memory_space=pltpu.SMEM)] + [here] * count,
        out_specs=[here] * 8,
        out_shape=[jax.ShapeDtypeStruct((count * size, D), BF16) for size in SIZES]
        + [jax.ShapeDtypeStruct((count, TOK, 4 * CAP), BF16)] * 2,
    )(experts, *messages)
    return outs[:6], outs[6:]


def combine_kernel(count, high, low, *refs):
    parts, outs = refs[:6], refs[6:]
    for i in range(count):
        rows = jnp.concatenate(
            [part[i * size : (i + 1) * size] for part, size in zip(parts, SIZES)], axis=0
        )
        total = jnp.dot(high[i], rows, preferred_element_type=F32)
        total = total + jnp.dot(low[i], rows, preferred_element_type=F32)
        outs[i][...] = total.astype(BF16)


def combine_rows(tables, parts):
    count = tables[0].shape[0]
    here = pl.BlockSpec(memory_space=pltpu.VMEM)
    return pl.pallas_call(
        lambda *refs: combine_kernel(count, *refs),
        in_specs=[here] * 8,
        out_specs=[here] * count,
        out_shape=[jax.ShapeDtypeStruct((TOK, D), BF16)] * count,
    )(*tables, *parts)


def ffn_kernel(count, *refs):
    new, far_new, core_new, core_far_new = refs[:4]
    others = refs[4:16]
    rows, outs = refs[16:22], refs[22:28]
    weights, held, result, weight_sem, row_sem, out_sem = refs[28:]
    share = 4 * CAP * count
    step = share // 2

    def moved(arrays, buffer, sem, inward):
        copies, begin = [], 0
        for i, (array, size) in enumerate(zip(arrays, SIZES)):
            place = pl.ds(begin, count * size)
            for h in range(2):
                far = array.at[:, pl.ds(h * HALF, HALF)]
                near = buffer.at[place, pl.ds((1 - h if i in SWAPPED else h) * HALF, HALF)]
                copies.append(pltpu.make_async_copy(*((far, near) if inward else (near, far)), sem.at[i, h]))
            begin += count * size
        return copies

    copies = []
    for m in range(3):
        for q, piece in enumerate((new, far_new, core_new, core_far_new)):
            place = pl.ds(q * HDEV, HDEV)
            copies.append(pltpu.make_async_copy(piece.at[m], weights.at[0, m, place], weight_sem.at[q, 0, m]))
            copies.append(
                pltpu.make_async_copy(others[3 * q + m], weights.at[1, m, place], weight_sem.at[q, 1, m])
            )
    copies += moved(rows, held, row_sem, True)
    for copy in copies:
        copy.start()
    for copy in copies:
        copy.wait()
    nt = (((1,), (1,)), ((), ()))

    def one_block(i, carry):
        begin = pl.multiple_of(i * step, step)
        x0, x1 = held[pl.ds(begin, step), :HALF], held[pl.ds(begin, step), HALF:]

        def project(m):
            return lax.dot_general(x0, weights[0, m], nt, preferred_element_type=F32) + lax.dot_general(
                x1, weights[1, m], nt, preferred_element_type=F32
            )

        hidden = (jax.nn.silu(project(0)) * project(1)).astype(BF16)
        for h in range(2):
            result[pl.ds(begin, step), h * HALF : (h + 1) * HALF] = jnp.dot(
                hidden, weights[h, 2], preferred_element_type=F32
            ).astype(BF16)
        return carry

    lax.fori_loop(0, 2, one_block, 0)
    copies = moved(outs, result, out_sem, False)
    for copy in copies:
        copy.start()
    for copy in copies:
        copy.wait()


def ffn(pieces, rows):
    count = rows[0].shape[0] // CAP
    share = 4 * CAP * count
    anywhere = pl.BlockSpec(memory_space=pl.ANY)
    return pl.pallas_call(
        lambda *refs: ffn_kernel(count, *refs),
        in_specs=[anywhere] * 22,
        out_specs=[anywhere] * 6,
        out_shape=[jax.ShapeDtypeStruct((count * size, D), BF16) for size in SIZES],
        scratch_shapes=[
            pltpu.VMEM((2, 3, HID, HALF), BF16),
            pltpu.VMEM((share, D), BF16),
            pltpu.VMEM((share, D), BF16),
            pltpu.SemaphoreType.DMA((4, 2, 3)),
            pltpu.SemaphoreType.DMA((6, 2)),
            pltpu.SemaphoreType.DMA((6, 2)),
        ],
    )(*pieces, *rows)


def halves(a, d, axis):
    left, right = jnp.split(a, 2, axis=axis)
    return jnp.where(d == 0, left, right), jnp.where(d == 0, right, left)


def plus(a, *others):
    total = a.astype(F32)
    for b in others:
        total = total + b.astype(F32)
    return total.astype(BF16)


MOVES = ((4, to_diagonal), (5, to_outer_diagonal), (2, to_y), (3, to_outer_y), (1, to_x))


def layer(tokens, routes, combine_weight, owner_plan, w_in, w_out, grad_in, grad_out, first_in, second_in, first_out, second_out):
    d = lax.axis_index("dp")
    yl, z, xp = lax.axis_index("yl"), lax.axis_index("z"), lax.axis_index("xp")
    experts = jnp.stack(
        [a * 16 + z * 2 + b for a, b in ((yl, xp), (yl, 1 - xp), (1 - yl, xp), (1 - yl, 1 - xp))]
    ).astype(jnp.int32)

    def permute(a, axis):
        return lax.ppermute(a, axis, SWAP)

    def spread_out(rows):
        got = list(rows)
        for i, move in MOVES:
            got[i] = move(rows[i])
        return got

    high = combine_weight.astype(BF16)
    low = (combine_weight - high.astype(F32)).astype(BF16)
    gap = jnp.zeros((TOK, 2), BF16)
    mine = jnp.concatenate(
        [*halves(tokens, d, 1), routes.astype(BF16), gap, high, gap, low, jnp.zeros((TOK, 106), BF16)], axis=1
    )
    up, down = [mine], [mine]
    for _ in range(3):
        up.append(along_z(up[-1], 1))
        down.append(along_z(down[-1], -1))
    across = jnp.concatenate([along_z(up[3][: TOK // 2], 1), along_z(down[3][TOK // 2 :], -1)], axis=0)

    got_in = permute(halves(grad_in[0], d, 2)[1], "dp")
    got_out = permute(halves(grad_out[0], d, 1)[1], "dp")
    new, moments, *apart = adam(
        d.reshape(1), w_in, w_out, grad_in, grad_out, got_in, got_out, first_in, second_in, first_out, second_out
    )

    def by_matrix(arrays, axis):
        return [permute(a, axis) for a in arrays]

    other = by_matrix(apart, "dp")
    far_new = permute(new, "xq")
    core_new = permute(new, "c")
    far_other = by_matrix(other, "xq")
    core_other = by_matrix(other, "c")
    core_far_new = permute(far_new, "c")
    core_far_other = by_matrix(far_other, "c")
    pieces = [new, far_new, core_new, core_far_new, *other, *far_other, *core_other, *core_far_other]

    near_rows, near_tables = select_rows(experts, [mine, up[1], down[1], up[2], down[2]])
    near_got = spread_out(near_rows)
    far_rows, far_tables = select_rows(experts, [up[3], down[3], across])
    far_got = spread_out(far_rows)

    plane, piece = ("yl", "xp"), (3 * GROUP_ROWS, 640)
    spread = exchange(moments.reshape(4, GROUPS, *piece), plane)
    spread = exchange(spread.transpose(1, 0, 2, 3), "z").reshape(NZ * 4, *piece)
    source = owner_plan.reshape(2, NZ, 2).transpose(1, 0, 2).reshape(NZ * 4)
    source = source % 16 // 2 * 4 + source // 16 * 2 + source % 2
    picked = spread.at[source].get(mode="promise_in_bounds").reshape(NZ, 4, *piece)
    landed = exchange(picked, "z").transpose(1, 0, 2, 3)
    landed = exchange(landed, plane)
    next_moments = unpack(landed.reshape(2, 2, GROUPS, *piece))

    far_done = ffn(pieces, far_got)
    far_back = spread_out(far_done)
    near_done = ffn(pieces, near_got)
    near_back = spread_out(near_done)

    below3, above3, opposite = combine_rows(far_tables, far_back)
    here, below1, above1, below2, above2 = combine_rows(near_tables, near_back)
    rest = TOK // 2
    rising = along_z(opposite[:rest], 1)
    falling = along_z(opposite[rest:], -1)
    rising = jnp.concatenate([plus(above3[:rest], rising), above3[rest:]], axis=0)
    falling = jnp.concatenate([below3[:rest], plus(below3[rest:], falling)], axis=0)
    rising = along_z(rising, 1)
    falling = along_z(falling, -1)
    rising = along_z(plus(above2, rising), 1)
    falling = along_z(plus(below2, falling), -1)
    rising = along_z(plus(above1, rising), 1)
    falling = along_z(plus(below1, falling), -1)
    total = plus(here, rising, falling)
    combined = jnp.where(d == 0, total, jnp.concatenate([total[:, HALF:], total[:, :HALF]], axis=1))
    return (combined, *next_moments)


def solution(mesh):
    fine = Mesh(mesh.devices.reshape(YL, NZ, XP, XQ, CORES, NDP), AXES)
    expert = ("yl", "z", "xp", "xq", "c")
    in_specs = (
        P(AXES, None),
        P(AXES, None),
        P(AXES, None),
        P(),
        P(None, expert, "dp"),
        P(expert, "dp"),
        P("dp", None, expert, None),
        P("dp", expert, None),
        P(None, expert, "dp"),
        P(None, expert, "dp"),
        P(expert, "dp"),
        P(expert, "dp"),
    )
    out_specs = (
        P(AXES, None),
        P(None, expert, "dp"),
        P(None, expert, "dp"),
        P(expert, "dp"),
        P(expert, "dp"),
    )
    return jax.shard_map(layer, mesh=fine, in_specs=in_specs, out_specs=out_specs, check_vma=False)
```

```python
import jax
import jax.numpy as jnp
from jax import lax
from jax.experimental import pallas as pl
from jax.experimental.pallas import tpu as pltpu
from jax.sharding import Mesh
from jax.sharding import PartitionSpec as P


BETA_ONE = 0.9
BETA_TWO = 0.95
LEARNING_RATE = 0.005
EPSILON = 1e-08
CORRECT_FIRST = 1.0 / (1.0 - 0.9**10)
CORRECT_SECOND = 1.0 / (1.0 - 0.95**10)

YL, NZ, XP, XQ, CORES, NDP = 2, 8, 2, 2, 2, 2
AXES = ("yl", "z", "xp", "xq", "c", "dp")
TOK, TOP, D, HALF, HDEV, CAP = 128, 6, 2560, 1280, 192, 32
MOVERS = 3
GROUPS, GROUP_ROWS = 8, 24
HID = 4 * HDEV
SIZES = (CAP, CAP, CAP // 2, CAP // 2, CAP // 2, CAP // 2)
SWAPPED = (3, 5)
SWAP = [(0, 1), (1, 0)]
X_FAR = [(0, 3), (3, 0), (1, 2), (2, 1)]
DIAGONAL = [(yl * 4 + a, (1 - yl) * 4 + b) for yl in range(2) for a, b in X_FAR]
OUTER = [(0, 3), (3, 0), (1, 2), (2, 1)]
OUTER_DIAGONAL = [(a * 2 + dp, b * 2 + 1 - dp) for a, b in DIAGONAL for dp in range(2)]

BF16, F32 = jnp.bfloat16, jnp.float32


def to_x(a):
    return lax.ppermute(a, ("xp", "xq"), X_FAR)


def to_y(a):
    return lax.ppermute(a, "yl", SWAP)


def to_diagonal(a):
    return lax.ppermute(a, ("yl", "xp", "xq"), DIAGONAL)


def to_outer_y(a):
    return lax.ppermute(a, ("yl", "dp"), OUTER)


def to_outer_diagonal(a):
    return lax.ppermute(a, ("yl", "xp", "xq", "dp"), OUTER_DIAGONAL)


def exchange(a, axes):
    return lax.all_to_all(a, axes, 0, 0, tiled=True)


def along_z(a, step):
    return lax.ppermute(a, "z", [(i, (i + step) % NZ) for i in range(NZ)])


def adam_kernel(d_ref, w_in, w_out, g_in, g_out, got_in, got_out, f_in, s_in, f_out, s_out, new, moments, *apart):
    for m in range(3):
        w, ga, gb, f, s = (
            (w_in[m], g_in[0, m], got_in[m], f_in[m], s_in[m])
            if m < 2
            else (w_out[...], g_out[0], got_out[...], f_out[...], s_out[...])
        )
        g = ga.astype(F32) + gb.astype(F32)
        first = BETA_ONE * f.astype(F32) + (1.0 - BETA_ONE) * g
        second = BETA_TWO * s.astype(F32) + (1.0 - BETA_TWO) * g * g
        stepped = w.astype(F32) - LEARNING_RATE * (first * CORRECT_FIRST) / (
            jnp.sqrt(second * CORRECT_SECOND) + EPSILON
        )
        new[m] = apart[m][...] = stepped.astype(BF16)
        for i, moment in enumerate((first, second)):
            for h in range(2):
                moments[i, h, 0, m * GROUP_ROWS : (m + 1) * GROUP_ROWS] = moment[
                    :, h * 640 : (h + 1) * 640
                ].astype(BF16)


def adam(d, w_in, w_out, g_in, g_out, got_in, got_out, f_in, s_in, f_out, s_out):
    block = GROUP_ROWS
    three = pl.BlockSpec((2, block, HALF), lambda i, d: (0, i, 0))
    two = pl.BlockSpec((block, HALF), lambda i, d: (i, 0))
    return pl.pallas_call(
        adam_kernel,
        grid_spec=pltpu.PrefetchScalarGridSpec(
            num_scalar_prefetch=1,
            grid=(GROUPS,),
            in_specs=[
                three,
                two,
                pl.BlockSpec((1, 2, block, HALF), lambda i, d: (0, 0, i, d[0])),
                pl.BlockSpec((1, block, HALF), lambda i, d: (0, i, d[0])),
                three,
                two,
                three,
                three,
                two,
                two,
            ],
            out_specs=[
                pl.BlockSpec((3, block, HALF), lambda i, d: (0, i, 0)),
                pl.BlockSpec((2, 2, 1, 3 * block, 640), lambda i, d: (0, 0, i, 0, 0)),
                two,
                two,
                two,
            ],
        ),
        out_shape=[
            jax.ShapeDtypeStruct((3, HDEV, HALF), BF16),
            jax.ShapeDtypeStruct((2, 2, GROUPS, 3 * block, 640), BF16),
        ]
        + [jax.ShapeDtypeStruct((HDEV, HALF), BF16)] * 3,
        name="adam",
    )(d, w_in, w_out, g_in, g_out, got_in, got_out, f_in, s_in, f_out, s_out)


def plan_kernel(place, plan, outgoing, crossing, incoming, flags, rank, mine):
    def where_of(expert):
        return expert % 16 // 2, expert // 16 * 2 + expert % 2

    overflow = jnp.int32(0)
    for z in range(NZ):
        seen = jnp.int32(0)
        for p in range(4):
            rank[z * 4 + p] = seen
            expert = p // 2 * 16 + z * 2 + p % 2
            seen = seen + (plan[expert] != expert).astype(jnp.int32)
        overflow = jnp.maximum(overflow, (seen > MOVERS).astype(jnp.int32))
    for i in range(NZ * MOVERS):
        crossing[i] = 0
    for j in range(MOVERS):
        mine[j] = 0
    for z in range(NZ):
        for p in range(4):
            expert = p // 2 * 16 + z * 2 + p % 2
            slot = rank[z * 4 + p]
            counts = (plan[expert] != expert) & (slot < MOVERS)
            from_z, from_p = where_of(plan[expert])
            source = from_z * MOVERS + jnp.minimum(rank[from_z * 4 + from_p], MOVERS - 1)
            crossing[jnp.where(counts, z * MOVERS + slot, NZ * MOVERS)] = source
            mine[jnp.where(counts & (place[0] == z), slot, MOVERS)] = p
    for z in range(NZ):
        for j in range(MOVERS):
            outgoing[z * MOVERS + j] = mine[j] * NZ + z
        for p in range(4):
            incoming[p * NZ + z] = z * MOVERS + jnp.minimum(rank[place[0] * 4 + p], MOVERS - 1)
    expert = place[1]
    flags[0] = (plan[expert] != expert).astype(jnp.int32)
    flags[1] = overflow


def plan_tables(place, plan):
    scalar = pl.BlockSpec(memory_space=pltpu.SMEM)
    return pl.pallas_call(
        plan_kernel,
        in_specs=[scalar] * 2,
        out_specs=[scalar] * 4,
        out_shape=[
            jax.ShapeDtypeStruct((n,), jnp.int32) for n in (NZ * MOVERS, NZ * MOVERS + 1, NZ * 4, 2)
        ],
        scratch_shapes=[pltpu.SMEM((NZ * 4,), jnp.int32), pltpu.SMEM((MOVERS + 1,), jnp.int32)],
        name="plan",
    )(place, plan)


def unpack_kernel(flags, landed, kept, f_in, s_in, f_out, s_out):
    moves = flags[0] != 0
    for i, (inward, outward) in enumerate(((f_in, f_out), (s_in, s_out))):
        for m in range(3):
            for h in range(2):
                rows = slice(m * GROUP_ROWS, (m + 1) * GROUP_ROWS)
                part = jnp.where(moves, landed[i, h, 0, rows], kept[i, h, 0, rows])
                if m < 2:
                    inward[m, :, h * 640 : (h + 1) * 640] = part
                else:
                    outward[:, h * 640 : (h + 1) * 640] = part


def unpack(flags, landed, kept):
    block = GROUP_ROWS
    three = pl.BlockSpec((2, block, HALF), lambda i, f: (0, i, 0))
    two = pl.BlockSpec((block, HALF), lambda i, f: (i, 0))
    inward = jax.ShapeDtypeStruct((2, HDEV, HALF), BF16)
    outward = jax.ShapeDtypeStruct((HDEV, HALF), BF16)
    return pl.pallas_call(
        unpack_kernel,
        grid_spec=pltpu.PrefetchScalarGridSpec(
            num_scalar_prefetch=1,
            grid=(GROUPS,),
            in_specs=[pl.BlockSpec((2, 2, 1, 3 * block, 640), lambda i, f: (0, 0, i, 0, 0))] * 2,
            out_specs=[three, three, two, two],
        ),
        out_shape=[inward, inward, outward, outward],
        name="unpack",
    )(flags, landed, kept)


def select_kernel(count, experts, *refs):
    messages, outs, (high, low) = refs[:count], refs[count : count + 6], refs[count + 6 :]
    lane = lax.broadcasted_iota(jnp.int32, (TOK, 4 * CAP), 1)
    row = lax.broadcasted_iota(jnp.int32, (TOK, TOK), 0)
    column = lax.broadcasted_iota(jnp.int32, (TOK, TOK), 1)
    before = jnp.where(column < row, 1.0, 0.0).astype(BF16)
    block, slot = lane // CAP, (lane % CAP).astype(F32)
    mine = jnp.where(
        block == 0, experts[0], jnp.where(block == 1, experts[1], jnp.where(block == 2, experts[2], experts[3]))
    ).astype(F32)
    for i, message in enumerate(messages):
        listing = message[:, D:].astype(F32)
        named = jnp.zeros((TOK, 4 * CAP), F32)
        weight = jnp.zeros((TOK, 4 * CAP), F32)
        for k in range(TOP):
            hit = listing[:, k : k + 1] == mine
            value = listing[:, 8 + k : 9 + k] + listing[:, 16 + k : 17 + k]
            named = jnp.where(hit, 1.0, named)
            weight = jnp.where(hit, value, weight)
        rank = jnp.dot(before, named.astype(BF16), preferred_element_type=F32)
        chosen = jnp.where(rank == slot, named, 0.0)
        table = chosen * weight
        top = table.astype(BF16)
        high[i] = top
        low[i] = (table - top.astype(F32)).astype(BF16)
        rows = lax.dot_general(
            chosen.astype(BF16), message[:, :D], (((0,), (0,)), ((), ())), preferred_element_type=F32
        ).astype(BF16)
        begin = 0
        for out, size in zip(outs, SIZES):
            out[i * size : (i + 1) * size] = rows[begin : begin + size]
            begin += size


def select_rows(experts, messages):
    count = len(messages)
    here = pl.BlockSpec(memory_space=pltpu.VMEM)
    outs = pl.pallas_call(
        lambda *refs: select_kernel(count, *refs),
        in_specs=[pl.BlockSpec(memory_space=pltpu.SMEM)] + [here] * count,
        out_specs=[here] * 8,
        out_shape=[jax.ShapeDtypeStruct((count * size, D), BF16) for size in SIZES]
        + [jax.ShapeDtypeStruct((count, TOK, 4 * CAP), BF16)] * 2,
    )(experts, *messages)
    return outs[:6], outs[6:]


def combine_kernel(count, high, low, *refs):
    parts, outs = refs[:6], refs[6:]
    for i in range(count):
        rows = jnp.concatenate(
            [part[i * size : (i + 1) * size] for part, size in zip(parts, SIZES)], axis=0
        )
        total = jnp.dot(high[i], rows, preferred_element_type=F32)
        total = total + jnp.dot(low[i], rows, preferred_element_type=F32)
        outs[i][...] = total.astype(BF16)


def combine_rows(tables, parts):
    count = tables[0].shape[0]
    here = pl.BlockSpec(memory_space=pltpu.VMEM)
    return pl.pallas_call(
        lambda *refs: combine_kernel(count, *refs),
        in_specs=[here] * 8,
        out_specs=[here] * count,
        out_shape=[jax.ShapeDtypeStruct((TOK, D), BF16)] * count,
    )(*tables, *parts)


def ffn_kernel(count, *refs):
    new, far_new, core_new, core_far_new = refs[:4]
    others = refs[4:16]
    rows, outs = refs[16:22], refs[22:28]
    weights, held, result, weight_sem, row_sem, out_sem = refs[28:]
    share = 4 * CAP * count
    step = share // 2

    def moved(arrays, buffer, sem, inward):
        copies, begin = [], 0
        for i, (array, size) in enumerate(zip(arrays, SIZES)):
            place = pl.ds(begin, count * size)
            for h in range(2):
                far = array.at[:, pl.ds(h * HALF, HALF)]
                near = buffer.at[place, pl.ds((1 - h if i in SWAPPED else h) * HALF, HALF)]
                copies.append(pltpu.make_async_copy(*((far, near) if inward else (near, far)), sem.at[i, h]))
            begin += count * size
        return copies

    copies = []
    for m in range(3):
        for q, piece in enumerate((new, far_new, core_new, core_far_new)):
            place = pl.ds(q * HDEV, HDEV)
            copies.append(pltpu.make_async_copy(piece.at[m], weights.at[0, m, place], weight_sem.at[q, 0, m]))
            copies.append(
                pltpu.make_async_copy(others[3 * q + m], weights.at[1, m, place], weight_sem.at[q, 1, m])
            )
    copies += moved(rows, held, row_sem, True)
    for copy in copies:
        copy.start()
    for copy in copies:
        copy.wait()
    nt = (((1,), (1,)), ((), ()))

    def one_block(i, carry):
        begin = pl.multiple_of(i * step, step)
        x0, x1 = held[pl.ds(begin, step), :HALF], held[pl.ds(begin, step), HALF:]

        def project(m):
            return lax.dot_general(x0, weights[0, m], nt, preferred_element_type=F32) + lax.dot_general(
                x1, weights[1, m], nt, preferred_element_type=F32
            )

        hidden = (jax.nn.silu(project(0)) * project(1)).astype(BF16)
        for h in range(2):
            result[pl.ds(begin, step), h * HALF : (h + 1) * HALF] = jnp.dot(
                hidden, weights[h, 2], preferred_element_type=F32
            ).astype(BF16)
        return carry

    lax.fori_loop(0, 2, one_block, 0)
    copies = moved(outs, result, out_sem, False)
    for copy in copies:
        copy.start()
    for copy in copies:
        copy.wait()


def ffn(pieces, rows):
    count = rows[0].shape[0] // CAP
    share = 4 * CAP * count
    anywhere = pl.BlockSpec(memory_space=pl.ANY)
    return pl.pallas_call(
        lambda *refs: ffn_kernel(count, *refs),
        in_specs=[anywhere] * 22,
        out_specs=[anywhere] * 6,
        out_shape=[jax.ShapeDtypeStruct((count * size, D), BF16) for size in SIZES],
        scratch_shapes=[
            pltpu.VMEM((2, 3, HID, HALF), BF16),
            pltpu.VMEM((share, D), BF16),
            pltpu.VMEM((share, D), BF16),
            pltpu.SemaphoreType.DMA((4, 2, 3)),
            pltpu.SemaphoreType.DMA((6, 2)),
            pltpu.SemaphoreType.DMA((6, 2)),
        ],
    )(*pieces, *rows)


def halves(a, d, axis):
    left, right = jnp.split(a, 2, axis=axis)
    return jnp.where(d == 0, left, right), jnp.where(d == 0, right, left)


def plus(a, *others):
    total = a.astype(F32)
    for b in others:
        total = total + b.astype(F32)
    return total.astype(BF16)


MOVES = ((4, to_diagonal), (5, to_outer_diagonal), (2, to_y), (3, to_outer_y), (1, to_x))


def layer(tokens, routes, combine_weight, owner_plan, w_in, w_out, grad_in, grad_out, first_in, second_in, first_out, second_out):
    d = lax.axis_index("dp")
    yl, z, xp = lax.axis_index("yl"), lax.axis_index("z"), lax.axis_index("xp")
    experts = jnp.stack(
        [a * 16 + z * 2 + b for a, b in ((yl, xp), (yl, 1 - xp), (1 - yl, xp), (1 - yl, 1 - xp))]
    ).astype(jnp.int32)

    def permute(a, axis):
        return lax.ppermute(a, axis, SWAP)

    def spread_out(rows):
        got = list(rows)
        for i, move in MOVES:
            got[i] = move(rows[i])
        return got

    high = combine_weight.astype(BF16)
    low = (combine_weight - high.astype(F32)).astype(BF16)
    gap = jnp.zeros((TOK, 2), BF16)
    mine = jnp.concatenate(
        [*halves(tokens, d, 1), routes.astype(BF16), gap, high, gap, low, jnp.zeros((TOK, 106), BF16)], axis=1
    )
    up, down = [mine], [mine]
    for _ in range(3):
        up.append(along_z(up[-1], 1))
        down.append(along_z(down[-1], -1))
    across = jnp.concatenate([along_z(up[3][: TOK // 2], 1), along_z(down[3][TOK // 2 :], -1)], axis=0)

    got_in = permute(halves(grad_in[0], d, 2)[1], "dp")
    got_out = permute(halves(grad_out[0], d, 1)[1], "dp")
    new, moments, *apart = adam(
        d.reshape(1), w_in, w_out, grad_in, grad_out, got_in, got_out, first_in, second_in, first_out, second_out
    )

    def by_matrix(arrays, axis):
        return [permute(a, axis) for a in arrays]

    other = by_matrix(apart, "dp")
    far_new = permute(new, "xq")
    core_new = permute(new, "c")
    far_other = by_matrix(other, "xq")
    core_other = by_matrix(other, "c")
    core_far_new = permute(far_new, "c")
    core_far_other = by_matrix(far_other, "c")
    pieces = [new, far_new, core_new, core_far_new, *other, *far_other, *core_other, *core_far_other]

    near_rows, near_tables = select_rows(experts, [mine, up[1], down[1], up[2], down[2]])
    near_got = spread_out(near_rows)
    far_rows, far_tables = select_rows(experts, [up[3], down[3], across])
    far_got = spread_out(far_rows)

    plane, piece = ("yl", "xp"), (3 * GROUP_ROWS, 640)

    def rows_at(array, index, *shape):
        return array.reshape(-1, *piece).at[index].get(mode="promise_in_bounds").reshape(*shape, *piece)

    place = jnp.stack([z, yl * 16 + z * 2 + xp]).astype(jnp.int32)
    outgoing, crossing, incoming, flags = plan_tables(place, owner_plan)
    spread = exchange(moments.reshape(4, GROUPS, *piece), plane)
    spread = exchange(rows_at(spread, outgoing, NZ, MOVERS), "z")
    landed = exchange(rows_at(spread, crossing[: NZ * MOVERS], NZ, MOVERS), "z")
    landed = exchange(rows_at(landed, incoming, 4, NZ), plane)

    def all_move(landed, moments):
        everywhere = ("yl", "z", "xp")
        spread = exchange(moments.reshape(32, *piece), everywhere)
        return exchange(rows_at(spread, owner_plan, 32), everywhere).reshape(landed.shape)

    landed = lax.cond(flags[1] != 0, all_move, lambda landed, moments: landed, landed, moments)
    next_moments = unpack(flags, landed.reshape(2, 2, GROUPS, *piece), moments)

    far_done = ffn(pieces, far_got)
    far_back = spread_out(far_done)
    near_done = ffn(pieces, near_got)
    near_back = spread_out(near_done)

    below3, above3, opposite = combine_rows(far_tables, far_back)
    here, below1, above1, below2, above2 = combine_rows(near_tables, near_back)
    rest = TOK // 2
    rising = along_z(opposite[:rest], 1)
    falling = along_z(opposite[rest:], -1)
    rising = jnp.concatenate([plus(above3[:rest], rising), above3[rest:]], axis=0)
    falling = jnp.concatenate([below3[:rest], plus(below3[rest:], falling)], axis=0)
    rising = along_z(rising, 1)
    falling = along_z(falling, -1)
    rising = along_z(plus(above2, rising), 1)
    falling = along_z(plus(below2, falling), -1)
    rising = along_z(plus(above1, rising), 1)
    falling = along_z(plus(below1, falling), -1)
    total = plus(here, rising, falling)
    combined = jnp.where(d == 0, total, jnp.concatenate([total[:, HALF:], total[:, :HALF]], axis=1))
    return (combined, *next_moments)


def solution(mesh):
    fine = Mesh(mesh.devices.reshape(YL, NZ, XP, XQ, CORES, NDP), AXES)
    expert = ("yl", "z", "xp", "xq", "c")
    in_specs = (
        P(AXES, None),
        P(AXES, None),
        P(AXES, None),
        P(),
        P(None, expert, "dp"),
        P(expert, "dp"),
        P("dp", None, expert, None),
        P("dp", expert, None),
        P(None, expert, "dp"),
        P(None, expert, "dp"),
        P(expert, "dp"),
        P(expert, "dp"),
    )
    out_specs = (
        P(AXES, None),
        P(None, expert, "dp"),
        P(None, expert, "dp"),
        P(expert, "dp"),
        P(expert, "dp"),
    )
    return jax.shard_map(layer, mesh=fine, in_specs=in_specs, out_specs=out_specs, check_vma=False)
```
